32 devices in a mesh: grp: 2 (over core), dev: 16 (over z, y, x).
Axes of the slice: x: 2, y: 2, z: 4, core: 2. Of those that a mesh axis runs over, the one named last changes fastest.
Arguments:
- accum: float32 [4096, 24, 128], P(('grp', 'dev')), may hold values from -48 to 48
- step_count: int32 [24], replicated, may hold values from 1 to 12
- stretch_slot: int32 [4096], replicated, may hold values from 0 to 4095, as said below
- span_length: int32 [32], replicated, may hold values from 1 to 256, 4096 in all
- wet_mask: int32 [8192], P(('grp', 'dev')), may hold values 0 or 1
Outputs:
- ocean_flux: float32 [8192, 24, 128], P(('grp', 'dev'))
The draws below stay inside these ranges and needn't reach their ends.
Inputs may be any that keep to these rules, and one draw needn't show every extreme that they name: `stretch_slot`: A permutation of the slots; any 32 consecutive row blocks lie on 32 different atmosphere devices (slot // 128). `span_length`: sums to 4096; some ocean device owns exactly 256 blocks. `wet_mask`: entries of slots beyond an ocean device's span are ignored.
All inputs are finite; a program needn't handle non-finite values.
Results may differ from the reference program's by a relative error of at most 0.000071.
Values sent between devices are 32-bit elements; how exact they have to be, the bound alone decides.
No kernel may reach another device: no remote copies, remote signals or barrier semaphores. Data moves between devices by JAX's collectives and lax.ppermute only.
A program may use at most 64 MiB of HBM per device.

```python
import math
import jax
import jax.numpy as jnp
import numpy as np

FIELDS = 24
CELLS = 128
BLOCKS_DEV = 128
DEVICE_COUNT = 32
ALL_BLOCKS = 4096
CAPACITY = 256


def draw_stretch_slot(key, part):
    devices = ALL_BLOCKS // BLOCKS_DEV
    first_key = jax.random.fold_in(key, 11)
    second_key = jax.random.fold_in(key, 12)
    dealing = jax.random.permutation(first_key, devices).astype(jnp.int32)
    rotation = jax.random.randint(second_key, (devices,), 0, BLOCKS_DEV).astype(jnp.int32)
    global_ids = jnp.arange(ALL_BLOCKS, dtype=jnp.int32)
    holder = dealing[global_ids % devices]
    local_slot = (global_ids // devices + rotation[holder]) % BLOCKS_DEV
    return (holder * BLOCKS_DEV + local_slot).astype(jnp.int32)


def set_ends(drawn, own_key, least, largest):
    extent = drawn.shape
    index_at = [jax.random.randint(jax.random.fold_in(own_key, axis), (), 0, extent[axis]) for axis in range(len(extent))]
    drawn = drawn.at[tuple(index_at)].set(least)
    longest = extent.index(max(extent))
    index_at[longest] = (index_at[longest] + 1) % extent[longest]
    return drawn.at[tuple(index_at)].set(largest)


def level_of(rng, shape, cuts, low, high):
    def one(axis_at, shards_of):
        draws = jax.random.uniform(jax.random.fold_in(jax.random.fold_in(rng, 6), axis_at), (shards_of,), jnp.float32, low / len(cuts), high / len(cuts))
        return jnp.repeat(jnp.exp(draws), shape[axis_at] // shards_of).reshape((-1,) + (1,) * (len(shape) - axis_at - 1))

    factor_of = one(*cuts[0])
    for cut in cuts[1:]:
        factor_of = factor_of * one(*cut)
    return factor_of


def profile(amount, total, limit, lean):
    weights = [(1 << 20) // math.isqrt(rank ** lean) + 1 for rank in range(2, amount + 1)]
    surplus, given = total - limit - (amount - 1), [1] * (amount - 1)
    while surplus > 0:
        free = [i for i in range(amount - 1) if given[i] < limit]
        mass, remaining = sum([weights[i] for i in free]), surplus
        for i in free:
            more = min(limit - given[i], max(1, remaining * weights[i] // mass), surplus)
            given[i] = given[i] + more
            surplus = surplus - more
    return np.array([limit] + given)


def ragged(rng, number_of, total, reach, slope):
    if number_of == 2:
        one = jax.random.randint(rng, (), max(1, total - reach), min(reach, total - 1) + 1)
        return jnp.stack([one, total - one])
    tallies = jnp.asarray(profile(number_of, total, reach, slope), jnp.int32)
    twos = (number_of - 1) // 2
    source_of, receiver = tallies[1:1 + 2 * twos:2], tallies[2:2 + 2 * twos:2]
    slack = jnp.minimum(source_of - 1, reach - receiver)
    moved = jax.random.randint(jax.random.fold_in(rng, 1), (twos,), 0, 1 << 20) % (slack + 1)
    tallies = tallies.at[1:1 + 2 * twos:2].set(source_of - moved).at[2:2 + 2 * twos:2].set(receiver + moved)
    return tallies[jax.random.permutation(jax.random.fold_in(rng, 2), number_of)]


def noise(rng, shape, scale, most, pieces=(), kind=jnp.bfloat16):
    values = jax.random.normal(rng, shape, jnp.float32) * scale
    if len(pieces) > 0:
        values = level_of(rng, shape, pieces, -0.22, 0.18) * values
    return jnp.clip(values, min=-most, max=most).astype(kind)


def setup_inputs(seed: int = 0) -> dict:
    keys = jax.random.split(jax.random.key(seed), 6)
    accum = noise(keys[0], (ALL_BLOCKS, FIELDS, CELLS), 8.0, 48.0, ((0, 32),), jnp.float32)
    step_count = set_ends(jax.random.randint(keys[1], (FIELDS,), 1, 13), jax.random.fold_in(keys[1], 1), 1, 12).astype(jnp.int32)
    stretch_slot = draw_stretch_slot(jax.random.fold_in(keys[5], 71), 0)
    span_length = ragged(keys[3], DEVICE_COUNT, ALL_BLOCKS, CAPACITY, 2).astype(jnp.int32)
    wet_mask = set_ends((jax.random.randint(keys[4], (DEVICE_COUNT * CAPACITY,), 0, 4) < 3).astype(jnp.int32), jax.random.fold_in(keys[4], 1), 0, 1)
    return dict(accum=accum, step_count=step_count, stretch_slot=stretch_slot, span_length=span_length, wet_mask=wet_mask)


def reference(accum, step_count, stretch_slot, span_length, wet_mask):
    span_end = jnp.cumsum(span_length).astype(jnp.int32)
    span_start = (span_end - span_length).astype(jnp.int32)
    global_ids = jnp.arange(ALL_BLOCKS, dtype=jnp.int32)
    owner = jnp.sum((span_end[None, :] <= global_ids[:, None]).astype(jnp.int32), axis=1).astype(jnp.int32)
    position = (owner * CAPACITY + global_ids - span_start[owner]).astype(jnp.int32)
    wet = (wet_mask[position] == 1).astype(jnp.float32)
    counts = step_count.astype(jnp.float32)
    masked = (accum[stretch_slot] / counts[None, :, None]) * wet[:, None, None]
    flat = jnp.transpose(masked, (1, 0, 2)).reshape(FIELDS, ALL_BLOCKS * CELLS)
    zero_col = jnp.zeros((FIELDS, 1), jnp.float32)
    before = jnp.concatenate([zero_col, flat[:, :-1]], axis=1)
    after_cells = jnp.concatenate([flat[:, 1:], zero_col], axis=1)
    smoothed = 0.25 * before + 0.5 * flat + 0.25 * after_cells
    smoothed = jnp.transpose(smoothed.reshape(FIELDS, ALL_BLOCKS, CELLS), (1, 0, 2)) * wet[:, None, None]
    result = jnp.zeros((DEVICE_COUNT * CAPACITY, FIELDS, CELLS), jnp.float32)
    return result.at[position].set(smoothed)
```

```python
import functools

import jax
import jax.numpy as jnp
from jax import lax
from jax.experimental import pallas as pl
from jax.experimental.pallas import tpu as pltpu
from jax.sharding import PartitionSpec as P

AXES = ("grp", "dev")
TILE = 8


def passed_along(value, axis, steps):
    count = lax.axis_size(axis)
    initial, last = (max(0, -steps), min(count, count - steps))
    return lax.ppermute(value, axis, [(source, source + steps) for source in range(initial, last)])


def pack_body(table, accum, counts, out, *, windows, owners, pair_most):
    _, fields, cells = accum.shape
    tiles = fields // TILE
    step = pl.program_id(0)
    per_step = out.shape[0]
    scale = jnp.broadcast_to(1.0 / counts[...].astype(jnp.float32), (fields, cells))
    lane = lax.broadcasted_iota(jnp.int32, (TILE, cells), 1)

    def block_at(window):
        local = table[jnp.clip(window, 0, windows - 1)]
        return accum[local] * scale

    for item in range(per_step):
        owner = step * per_step + item
        first = table[windows + owner]
        after = table[windows + owner + 1]
        for rank in range(pair_most):
            out[item, pl.ds(rank * fields, fields), :] = block_at(first + rank)
        left = block_at(first - 1)
        right = block_at(after)
        edge = jnp.zeros((TILE, cells), jnp.float32)
        for tile in range(tiles):
            rows = slice(tile * TILE, (tile + 1) * TILE)
            right_at = pltpu.roll(right[rows], tile, 1) if tile else right[rows]
            left_at = pltpu.roll(left[rows], cells - tile, 1) if tile else left[rows]
            edge = jnp.where(lane == tile, right_at, edge)
            edge = jnp.where(lane == cells - 1 - tile, left_at, edge)
        out[item, pl.ds(pair_most * fields, TILE), :] = edge


def pack(table, accum, counts, windows, owners, pair_most):
    blocks, fields, cells = accum.shape
    rows = pair_most * fields + TILE
    steps = 8
    per_step = owners // steps
    return pl.pallas_call(
        functools.partial(pack_body, windows=windows, owners=owners, pair_most=pair_most),
        out_shape=jax.ShapeDtypeStruct((owners, rows, cells), jnp.float32),
        grid_spec=pltpu.PrefetchScalarGridSpec(
            num_scalar_prefetch=1,
            grid=(steps,),
            in_specs=[
                pl.BlockSpec((blocks, fields, cells), lambda i, t: (0, 0, 0)),
                pl.BlockSpec((fields, 1), lambda i, t: (0, 0)),
            ],
            out_specs=pl.BlockSpec((per_step, rows, cells), lambda i, t: (i, 0, 0)),
        ),
        name="pack",
    )(table, accum, counts)


def place_body(info, received, out, *, capacity):
    chunk, fields, cells = out.shape
    tiles = fields // TILE
    base = pl.program_id(0) * chunk
    left_row = pl.multiple_of(info[2 * capacity], TILE)
    right_row = pl.multiple_of(info[2 * capacity + 1], TILE)
    left_wet = info[2 * capacity + 2].astype(jnp.float32)
    right_wet = info[2 * capacity + 3].astype(jnp.float32)
    last = info[2 * capacity + 4]
    left_tile = received[pl.ds(left_row, TILE), :] * left_wet
    right_tile = received[pl.ds(right_row, TILE), :] * right_wet
    left_edge = jnp.concatenate([pltpu.roll(left_tile, tile + 1, 1) for tile in range(tiles)], axis=0)
    right_edge = jnp.concatenate(
        [pltpu.roll(right_tile, cells - 1 - tile, 1) for tile in range(tiles)], axis=0
    )
    lane = lax.broadcasted_iota(jnp.int32, (fields, cells), 1)

    def masked_at(slot):
        row = pl.multiple_of(info[slot], TILE)
        wet = info[capacity + slot].astype(jnp.float32)
        return received[pl.ds(row, fields), :] * wet, wet

    before_block, _ = masked_at(jnp.maximum(base - 1, 0))
    before = jnp.where(base == 0, left_edge, pltpu.roll(before_block, 1, 1))
    block, wet = masked_at(base)
    ahead = pltpu.roll(block, cells - 1, 1)
    for item in range(chunk):
        slot = base + item
        after_slot = jnp.minimum(slot + 1, capacity - 1) if item == chunk - 1 else slot + 1
        after_block, after_wet = masked_at(after_slot)
        behind = pltpu.roll(block, 1, 1)
        after_ahead = pltpu.roll(after_block, cells - 1, 1)
        coming = jnp.where(slot == last, right_edge, after_ahead)
        sides = jnp.where(lane == 0, before, behind) + jnp.where(lane == cells - 1, coming, ahead)
        out[item] = (0.25 * sides + 0.5 * block) * wet
        before, block, wet, ahead = behind, after_block, after_wet, after_ahead


def place(info, received, capacity, fields, cells):
    steps = 8
    chunk = capacity // steps
    return pl.pallas_call(
        functools.partial(place_body, capacity=capacity),
        out_shape=jax.ShapeDtypeStruct((capacity, fields, cells), jnp.float32),
        grid_spec=pltpu.PrefetchScalarGridSpec(
            num_scalar_prefetch=1,
            grid=(steps,),
            in_specs=[pl.BlockSpec(received.shape, lambda i, t: (0, 0))],
            out_specs=pl.BlockSpec((chunk, fields, cells), lambda i, t: (i, 0, 0)),
        ),
        name="place",
    )(info, received)


def on_device(accum, step_count, stretch_slot, span_length, wet_mask):
    devices = lax.axis_size(AXES)
    me = lax.axis_index(AXES)
    blocks_dev, fields, cells = accum.shape
    capacity = wet_mask.shape[0]
    pair_most = capacity // devices
    all_blocks = stretch_slot.shape[0]
    windows = all_blocks // devices
    rows = pair_most * fields + TILE

    by_window = stretch_slot.reshape(windows, devices)
    here = by_window // blocks_dev == me
    ids = jnp.arange(all_blocks, dtype=jnp.int32).reshape(windows, devices)
    local = jnp.sum(jnp.where(here, by_window % blocks_dev, 0), axis=1)
    my_global = jnp.sum(jnp.where(here, ids, 0), axis=1)
    owner_ids = jnp.arange(devices, dtype=jnp.int32)
    edge_ids = jnp.arange(devices + 1, dtype=jnp.int32)
    starts = jnp.sum(jnp.where(owner_ids[None, :] < edge_ids[:, None], span_length[None, :], 0), axis=1)
    first_window = jnp.sum((my_global[None, :] < starts[:, None]).astype(jnp.int32), axis=1)
    table = jnp.concatenate([local, first_window])
    sendbuf = pack(table, accum, step_count.reshape(fields, 1), windows, devices, pair_most)
    received = lax.all_to_all(sendbuf, AXES, split_axis=0, concat_axis=0, tiled=True)
    received = received.reshape(devices * rows, cells)

    length = span_length[me]
    start = jnp.sum(jnp.where(owner_ids < me, span_length, 0))
    slots = jnp.arange(capacity, dtype=jnp.int32)
    valid = slots < length
    wet = jnp.where(valid & (wet_mask == 1), 1, 0)
    left_wet = passed_along(wet[length - 1], AXES, 1)
    right_wet = passed_along(wet[0], AXES, -1)
    padded = jnp.pad(stretch_slot, (1, capacity + 1))
    around = lax.dynamic_slice_in_dim(padded, start, capacity + 2) // blocks_dev
    sender = around[1:-1]
    opening = start // devices
    opening_senders = lax.dynamic_slice_in_dim(stretch_slot, opening * devices, devices) // blocks_dev
    skipped = (opening_senders[None, :] == sender[:, None]) & (owner_ids < start % devices)[None, :]
    rank = (start + slots) // devices - opening - jnp.sum(skipped.astype(jnp.int32), axis=1)
    row_of = jnp.where(valid, sender * rows + rank * fields, 0)
    edge_row = pair_most * fields
    left_row = around[0] * rows + edge_row
    right_row = jnp.sum(jnp.where(slots == length - 1, around[2:], 0)) * rows + edge_row
    ends = jnp.stack([left_row, right_row, left_wet, right_wet, length - 1])
    info = jnp.concatenate([row_of, wet, ends])
    return place(info, received, capacity, fields, cells)


def solution(mesh):
    return jax.shard_map(
        on_device,
        mesh=mesh,
        in_specs=(P(AXES, None, None), P(), P(), P(), P(AXES)),
        out_specs=P(AXES, None, None),
        check_vma=False,
    )
```

```python
import functools

import jax
import jax.numpy as jnp
from jax import lax
from jax.experimental import pallas as pl
from jax.experimental.pallas import tpu as pltpu
from jax.sharding import PartitionSpec as P

AXES = ("grp", "dev")
TILE = 8


def passed_along(value, axis, steps):
    count = lax.axis_size(axis)
    initial, last = (max(0, -steps), min(count, count - steps))
    return lax.ppermute(value, axis, [(source, source + steps) for source in range(initial, last)])


def pack_body(table, accum, out, *, windows, pair_most):
    fields = accum.shape[1]

    def one_owner(owner, carry):
        first = table[windows + owner]
        for rank in range(pair_most):
            local = table[jnp.minimum(first + rank, windows - 1)]
            out[owner, pl.ds(rank * fields, fields), :] = accum[local]
        return carry

    lax.fori_loop(0, out.shape[0], one_owner, 0, unroll=2)


def pack(table, accum, windows, owners, pair_most):
    blocks, fields, cells = accum.shape
    return pl.pallas_call(
        functools.partial(pack_body, windows=windows, pair_most=pair_most),
        out_shape=jax.ShapeDtypeStruct((owners, pair_most * fields, cells), jnp.float32),
        in_specs=[
            pl.BlockSpec(memory_space=pltpu.SMEM),
            pl.BlockSpec(memory_space=pltpu.VMEM),
        ],
        out_specs=pl.BlockSpec(memory_space=pltpu.VMEM),
        name="pack",
    )(table, accum)


def edges_body(table, held, accum, out, *, windows, owners):
    _, fields, cells = accum.shape
    tiles = fields // TILE
    group = cells // tiles
    half = out.shape[0] // 2
    lane = lax.broadcasted_iota(jnp.int32, (TILE, cells), 1)
    out[...] = jnp.zeros(out.shape, jnp.float32)

    def one_owner(owner, carry):
        first = table[windows + owner]
        after = table[windows + owner + 1]
        row = pl.multiple_of(owner // group * TILE, TILE)
        at = owner % group * tiles
        sides = (
            (0, first - 1, held[owner], cells - 1),
            (half, after, held[owners + 1 + owner + 1], 0),
        )
        for base, window, has, cell in sides:
            block = accum[table[jnp.clip(window, 0, windows - 1)]]
            for tile in range(tiles):
                turned = pltpu.roll(block[tile * TILE:(tile + 1) * TILE], (at + tile + cells - cell) % cells, 1)
                kept = (lane == at + tile) & (has > 0)
                rows = pl.ds(pl.multiple_of(base + row, TILE), TILE)
                out[rows, :] = jnp.where(kept, turned, out[rows, :])
        return carry

    lax.fori_loop(0, owners, one_owner, 0)


def edges(table, held, accum, windows, owners):
    _, fields, cells = accum.shape
    group = cells // (fields // TILE)
    height = 2 * TILE * pl.cdiv(owners, group)
    return pl.pallas_call(
        functools.partial(edges_body, windows=windows, owners=owners),
        out_shape=jax.ShapeDtypeStruct((height, cells), jnp.float32),
        in_specs=[
            pl.BlockSpec(memory_space=pltpu.SMEM),
            pl.BlockSpec(memory_space=pltpu.SMEM),
            pl.BlockSpec(memory_space=pltpu.VMEM),
        ],
        out_specs=pl.BlockSpec(memory_space=pltpu.VMEM),
        name="edges",
    )(table, held, accum)


def place_body(info, received, ends, counts, out, *, capacity):
    chunk, fields, cells = out.shape
    tiles = fields // TILE
    base = pl.program_id(0) * chunk
    half = ends.shape[0] // 2
    left_wet = info[2 * capacity].astype(jnp.float32)
    right_wet = info[2 * capacity + 1].astype(jnp.float32)
    last = info[2 * capacity + 2]
    end_row = pl.multiple_of(info[2 * capacity + 3], TILE)
    end_lane = info[2 * capacity + 4]
    left_tile = ends[pl.ds(end_row, TILE), :] * left_wet
    right_tile = ends[pl.ds(pl.multiple_of(half + end_row, TILE), TILE), :] * right_wet
    left_edge = jnp.concatenate(
        [pltpu.roll(left_tile, (cells - end_lane - tile) % cells, 1) for tile in range(tiles)], axis=0
    )
    right_edge = jnp.concatenate(
        [pltpu.roll(right_tile, cells - 1 - end_lane - tile, 1) for tile in range(tiles)], axis=0
    )
    lane = lax.broadcasted_iota(jnp.int32, (fields, cells), 1)
    half_scale = jnp.broadcast_to(0.5 / counts[...].astype(jnp.float32), (fields, cells))

    def masked_at(slot):
        row = pl.multiple_of(info[slot], TILE)
        wet = info[capacity + slot].astype(jnp.float32)
        return received[pl.ds(row, fields), :] * wet, wet

    before_block, _ = masked_at(jnp.maximum(base - 1, 0))
    before = jnp.where(base == 0, left_edge, pltpu.roll(before_block, 1, 1))
    block, wet = masked_at(base)
    ahead = pltpu.roll(block, cells - 1, 1)
    for item in range(chunk):
        slot = base + item
        after_slot = jnp.minimum(slot + 1, capacity - 1) if item == chunk - 1 else slot + 1
        after_block, after_wet = masked_at(after_slot)
        behind = pltpu.roll(block, 1, 1)
        after_ahead = pltpu.roll(after_block, cells - 1, 1)
        coming = jnp.where(slot == last, right_edge, after_ahead)
        sides = jnp.where(lane == 0, before, behind) + jnp.where(lane == cells - 1, coming, ahead)
        out[item] = (0.5 * sides + block) * (half_scale * wet)
        before, block, wet, ahead = behind, after_block, after_wet, after_ahead


def place(info, received, ends, counts, capacity, fields, cells):
    steps = 8
    chunk = capacity // steps
    whole = pl.BlockSpec(memory_space=pltpu.VMEM)
    return pl.pallas_call(
        functools.partial(place_body, capacity=capacity),
        out_shape=jax.ShapeDtypeStruct((capacity, fields, cells), jnp.float32),
        grid=(steps,),
        in_specs=[pl.BlockSpec(memory_space=pltpu.SMEM), whole, whole, whole],
        out_specs=pl.BlockSpec((chunk, fields, cells), lambda i: (i, 0, 0)),
        name="place",
    )(info, received, ends, counts)


def on_device(accum, step_count, stretch_slot, span_length, wet_mask):
    devices = lax.axis_size(AXES)
    me = lax.axis_index(AXES)
    blocks_dev, fields, cells = accum.shape
    capacity = wet_mask.shape[0]
    pair_most = capacity // devices
    all_blocks = stretch_slot.shape[0]
    windows = all_blocks // devices
    rows = pair_most * fields

    by_window = stretch_slot.reshape(windows, devices)
    here = by_window // blocks_dev == me
    ids = jnp.arange(all_blocks, dtype=jnp.int32).reshape(windows, devices)
    local = jnp.sum(jnp.where(here, by_window % blocks_dev, 0), axis=1)
    my_global = jnp.sum(jnp.where(here, ids, 0), axis=1)
    owner_ids = jnp.arange(devices, dtype=jnp.int32)
    edge_ids = jnp.arange(devices + 1, dtype=jnp.int32)
    starts = jnp.sum(jnp.where(owner_ids[None, :] < edge_ids[:, None], span_length[None, :], 0), axis=1)
    first_window = jnp.sum((my_global[None, :] < starts[:, None]).astype(jnp.int32), axis=1)
    table = jnp.concatenate([local, first_window])
    sendbuf = pack(table, accum, windows, devices, pair_most)
    received = lax.all_to_all(sendbuf, AXES, split_axis=0, concat_axis=0, tiled=True)
    received = received.reshape(devices * rows, cells)

    offsets = jnp.concatenate([starts - 1, starts])
    held = jnp.sum((my_global[None, :] == offsets[:, None]).astype(jnp.int32), axis=1)
    ends = lax.psum(edges(table, held, accum, windows, devices), AXES)

    length = span_length[me]
    start = jnp.sum(jnp.where(owner_ids < me, span_length, 0))
    slots = jnp.arange(capacity, dtype=jnp.int32)
    valid = slots < length
    wet = jnp.where(valid & (wet_mask == 1), 1, 0)
    left_wet = passed_along(wet[length - 1], AXES, 1)
    right_wet = passed_along(wet[0], AXES, -1)
    padded = jnp.pad(stretch_slot, (0, capacity))
    sender = lax.dynamic_slice_in_dim(padded, start, capacity) // blocks_dev
    opening = start // devices
    opening_senders = lax.dynamic_slice_in_dim(stretch_slot, opening * devices, devices) // blocks_dev
    skipped = (opening_senders[None, :] == sender[:, None]) & (owner_ids < start % devices)[None, :]
    rank = (start + slots) // devices - opening - jnp.sum(skipped.astype(jnp.int32), axis=1)
    row_of = jnp.where(valid, sender * rows + rank * fields, 0)
    tiles = fields // TILE
    group = cells // tiles
    facts = jnp.stack([left_wet, right_wet, length - 1, me // group * TILE, me % group * tiles])
    info = jnp.concatenate([row_of, wet, facts])
    return place(info, received, ends, step_count.reshape(fields, 1), capacity, fields, cells)


def solution(mesh):
    return jax.shard_map(
        on_device,
        mesh=mesh,
        in_specs=(P(AXES, None, None), P(), P(), P(), P(AXES)),
        out_specs=P(AXES, None, None),
        check_vma=False,
    )
```

```python
import functools

import jax
import jax.numpy as jnp
from jax import lax
from jax.experimental import pallas as pl
from jax.experimental.pallas import tpu as pltpu
from jax.sharding import PartitionSpec as P

AXES = ("grp", "dev")
TILE = 8
SCRATCH_BYTES = 8 * 1024 * 1024


def passed_along(value, axis, steps):
    count = lax.axis_size(axis)
    initial, last = (max(0, -steps), min(count, count - steps))
    return lax.ppermute(value, axis, [(source, source + steps) for source in range(initial, last)])


def in_vmem(value):
    return pltpu.with_memory_space_constraint(value, pltpu.VMEM)


def pack_body(table, accum, out, *, windows, pair_most):
    _, fields, cells = accum.shape
    tiles = fields // TILE
    lane = lax.broadcasted_iota(jnp.int32, (TILE, cells), 1)

    def block_at(window):
        return accum[table[jnp.clip(window, 0, windows - 1)]]

    def one_owner(item, carry):
        owner = pl.program_id(0) * out.shape[0] + item
        first = table[windows + owner]
        for rank in range(pair_most):
            out[item, pl.ds(rank * fields, fields), :] = block_at(first + rank)
        left = block_at(first - 1)
        right = block_at(table[windows + owner + 1])
        edge = jnp.zeros((TILE, cells), jnp.float32)
        for tile in range(tiles):
            rows = slice(tile * TILE, (tile + 1) * TILE)
            right_at = pltpu.roll(right[rows], tile, 1) if tile else right[rows]
            left_at = pltpu.roll(left[rows], cells - tile, 1) if tile else left[rows]
            edge = jnp.where(lane == tile, right_at, edge)
            edge = jnp.where(lane == cells - 1 - tile, left_at, edge)
        out[item, pl.ds(pair_most * fields, TILE), :] = edge
        return carry

    lax.fori_loop(0, out.shape[0], one_owner, 0, unroll=4)


def pack(table, accum, windows, owners, pair_most):
    blocks, fields, cells = accum.shape
    rows = pair_most * fields + TILE
    steps = 8
    return pl.pallas_call(
        functools.partial(pack_body, windows=windows, pair_most=pair_most),
        out_shape=jax.ShapeDtypeStruct((owners, rows, cells), jnp.float32),
        grid=(steps,),
        in_specs=[
            pl.BlockSpec(memory_space=pltpu.SMEM),
            pl.BlockSpec(memory_space=pltpu.VMEM),
        ],
        out_specs=pl.BlockSpec((owners // steps, rows, cells), lambda i: (i, 0, 0)),
        compiler_params=pltpu.CompilerParams(vmem_limit_bytes=SCRATCH_BYTES),
        name="pack",
    )(table, in_vmem(accum))


def place_body(info, received, counts, out, *, capacity):
    chunk, fields, cells = out.shape
    tiles = fields // TILE
    base = pl.program_id(0) * chunk
    left_wet = info[2 * capacity].astype(jnp.float32)
    right_wet = info[2 * capacity + 1].astype(jnp.float32)
    last = info[2 * capacity + 2]
    left_row = pl.multiple_of(info[2 * capacity + 3], TILE)
    right_row = pl.multiple_of(info[2 * capacity + 4], TILE)
    left_tile = received[pl.ds(left_row, TILE), :] * left_wet
    right_tile = received[pl.ds(right_row, TILE), :] * right_wet
    left_edge = jnp.concatenate([pltpu.roll(left_tile, tile + 1, 1) for tile in range(tiles)], axis=0)
    right_edge = jnp.concatenate(
        [pltpu.roll(right_tile, cells - 1 - tile, 1) for tile in range(tiles)], axis=0
    )
    lane = lax.broadcasted_iota(jnp.int32, (fields, cells), 1)
    half_scale = jnp.broadcast_to(0.5 / counts[...].astype(jnp.float32), (fields, cells))

    def masked_at(slot):
        row = pl.multiple_of(info[slot], TILE)
        wet = info[capacity + slot].astype(jnp.float32)
        return received[pl.ds(row, fields), :] * wet, wet

    before_block, _ = masked_at(jnp.maximum(base - 1, 0))
    before = jnp.where(base == 0, left_edge, pltpu.roll(before_block, 1, 1))
    block, wet = masked_at(base)
    ahead = pltpu.roll(block, cells - 1, 1)
    for item in range(chunk):
        slot = base + item
        after_slot = jnp.minimum(slot + 1, capacity - 1) if item == chunk - 1 else slot + 1
        after_block, after_wet = masked_at(after_slot)
        behind = pltpu.roll(block, 1, 1)
        after_ahead = pltpu.roll(after_block, cells - 1, 1)
        coming = jnp.where(slot == last, right_edge, after_ahead)
        sides = jnp.where(lane == 0, before, behind) + jnp.where(lane == cells - 1, coming, ahead)
        out[item] = (0.5 * sides + block) * (half_scale * wet)
        before, block, wet, ahead = behind, after_block, after_wet, after_ahead


def place(info, received, counts, capacity, fields, cells):
    steps = 8
    chunk = capacity // steps
    whole = pl.BlockSpec(memory_space=pltpu.VMEM)
    return pl.pallas_call(
        functools.partial(place_body, capacity=capacity),
        out_shape=jax.ShapeDtypeStruct((capacity, fields, cells), jnp.float32),
        grid=(steps,),
        in_specs=[pl.BlockSpec(memory_space=pltpu.SMEM), whole, whole],
        out_specs=pl.BlockSpec((chunk, fields, cells), lambda i: (i, 0, 0)),
        compiler_params=pltpu.CompilerParams(vmem_limit_bytes=SCRATCH_BYTES),
        name="place",
    )(info, in_vmem(received), in_vmem(counts))


def on_device(accum, step_count, stretch_slot, span_length, wet_mask):
    devices = lax.axis_size(AXES)
    me = lax.axis_index(AXES)
    blocks_dev, fields, cells = accum.shape
    capacity = wet_mask.shape[0]
    pair_most = capacity // devices
    all_blocks = stretch_slot.shape[0]
    windows = all_blocks // devices
    rows = pair_most * fields + TILE

    by_window = stretch_slot.reshape(windows, devices)
    here = by_window // blocks_dev == me
    ids = jnp.arange(all_blocks, dtype=jnp.int32).reshape(windows, devices)
    local = jnp.sum(jnp.where(here, by_window % blocks_dev, 0), axis=1)
    my_global = jnp.sum(jnp.where(here, ids, 0), axis=1)
    owner_ids = jnp.arange(devices, dtype=jnp.int32)
    edge_ids = jnp.arange(devices + 1, dtype=jnp.int32)
    starts = jnp.sum(jnp.where(owner_ids[None, :] < edge_ids[:, None], span_length[None, :], 0), axis=1)
    first_window = jnp.sum((my_global[None, :] < starts[:, None]).astype(jnp.int32), axis=1)
    table = jnp.concatenate([local, first_window])
    sendbuf = pack(table, accum, windows, devices, pair_most)
    received = lax.all_to_all(sendbuf, AXES, split_axis=0, concat_axis=0, tiled=True)
    received = received.reshape(devices * rows, cells)

    length = span_length[me]
    start = jnp.sum(jnp.where(owner_ids < me, span_length, 0))
    slots = jnp.arange(capacity, dtype=jnp.int32)
    valid = slots < length
    wet = jnp.where(valid & (wet_mask == 1), 1, 0)
    left_wet = passed_along(wet[length - 1], AXES, 1)
    right_wet = passed_along(wet[0], AXES, -1)
    padded = jnp.pad(stretch_slot, (1, capacity + 1))
    around = lax.dynamic_slice_in_dim(padded, start, capacity + 2) // blocks_dev
    sender = around[1:-1]
    opening = start // devices
    opening_senders = lax.dynamic_slice_in_dim(stretch_slot, opening * devices, devices) // blocks_dev
    skipped = (opening_senders[None, :] == sender[:, None]) & (owner_ids < start % devices)[None, :]
    rank = (start + slots) // devices - opening - jnp.sum(skipped.astype(jnp.int32), axis=1)
    row_of = jnp.where(valid, sender * rows + rank * fields, 0)
    edge_row = pair_most * fields
    left_row = around[0] * rows + edge_row
    right_row = jnp.sum(jnp.where(slots == length - 1, around[2:], 0)) * rows + edge_row
    facts = jnp.stack([left_wet, right_wet, length - 1, left_row, right_row])
    info = jnp.concatenate([row_of, wet, facts])
    return place(info, received, step_count.reshape(fields, 1), capacity, fields, cells)


def solution(mesh):
    return jax.shard_map(
        on_device,
        mesh=mesh,
        in_specs=(P(AXES, None, None), P(), P(), P(), P(AXES)),
        out_specs=P(AXES, None, None),
        check_vma=False,
    )
```

```python
import functools

import jax
import jax.numpy as jnp
from jax import lax
from jax.experimental import pallas as pl
from jax.experimental.pallas import tpu as pltpu
from jax.sharding import PartitionSpec as P

AXES = ("grp", "dev")
TILE = 8
SCRATCH_BYTES = 8 * 1024 * 1024


def passed_along(value, axis, steps):
    count = lax.axis_size(axis)
    initial, last = (max(0, -steps), min(count, count - steps))
    return lax.ppermute(value, axis, [(source, source + steps) for source in range(initial, last)])


def in_vmem(value):
    return pltpu.with_memory_space_constraint(value, pltpu.VMEM)


def pack_body(table, accum, out, *, windows, pair_most):
    _, fields, cells = accum.shape
    tiles = fields // TILE
    lane = lax.broadcasted_iota(jnp.int32, (TILE, cells), 1)

    def block_at(window):
        return accum[table[jnp.clip(window, 0, windows - 1)]]

    def one_owner(item, carry):
        owner = pl.program_id(0) * out.shape[0] + item
        first = table[windows + owner]
        for rank in range(pair_most):
            out[item, pl.ds(rank * fields, fields), :] = block_at(first + rank)
        left = block_at(first - 1)
        right = block_at(table[windows + owner + 1])
        edge = jnp.zeros((TILE, cells), jnp.float32)
        for tile in range(tiles):
            rows = slice(tile * TILE, (tile + 1) * TILE)
            right_at = pltpu.roll(right[rows], tile, 1) if tile else right[rows]
            left_at = pltpu.roll(left[rows], cells - tile, 1) if tile else left[rows]
            edge = jnp.where(lane == tile, right_at, edge)
            edge = jnp.where(lane == cells - 1 - tile, left_at, edge)
        out[item, pl.ds(pair_most * fields, TILE), :] = edge
        return carry

    lax.fori_loop(0, out.shape[0], one_owner, 0, unroll=4)


def pack(table, accum, windows, owners, pair_most):
    blocks, fields, cells = accum.shape
    rows = pair_most * fields + TILE
    steps = 4
    return pl.pallas_call(
        functools.partial(pack_body, windows=windows, pair_most=pair_most),
        out_shape=pltpu.HBM((owners, rows, cells), jnp.float32),
        grid=(steps,),
        in_specs=[
            pl.BlockSpec(memory_space=pltpu.SMEM),
            pl.BlockSpec(memory_space=pltpu.VMEM),
        ],
        out_specs=pl.BlockSpec((owners // steps, rows, cells), lambda i: (i, 0, 0)),
        compiler_params=pltpu.CompilerParams(vmem_limit_bytes=SCRATCH_BYTES),
        name="pack",
    )(table, in_vmem(accum))


def place_body(info, received, counts, out, *, capacity):
    chunk, fields, cells = out.shape
    tiles = fields // TILE
    base = pl.program_id(0) * chunk
    left_wet = info[2 * capacity].astype(jnp.float32)
    right_wet = info[2 * capacity + 1].astype(jnp.float32)
    last = info[2 * capacity + 2]
    left_row = pl.multiple_of(info[2 * capacity + 3], TILE)
    right_row = pl.multiple_of(info[2 * capacity + 4], TILE)
    left_tile = received[pl.ds(left_row, TILE), :] * left_wet
    right_tile = received[pl.ds(right_row, TILE), :] * right_wet
    left_edge = jnp.concatenate([pltpu.roll(left_tile, tile + 1, 1) for tile in range(tiles)], axis=0)
    right_edge = jnp.concatenate(
        [pltpu.roll(right_tile, cells - 1 - tile, 1) for tile in range(tiles)], axis=0
    )
    lane = lax.broadcasted_iota(jnp.int32, (fields, cells), 1)
    half_scale = jnp.broadcast_to(0.5 / counts[...].astype(jnp.float32), (fields, cells))

    def masked_at(slot):
        row = pl.multiple_of(info[slot], TILE)
        wet = info[capacity + slot].astype(jnp.float32)
        return received[pl.ds(row, fields), :] * wet, wet

    before_block, _ = masked_at(jnp.maximum(base - 1, 0))
    before = jnp.where(base == 0, left_edge, pltpu.roll(before_block, 1, 1))
    block, wet = masked_at(base)
    ahead = pltpu.roll(block, cells - 1, 1)
    for item in range(chunk):
        slot = base + item
        after_slot = jnp.minimum(slot + 1, capacity - 1) if item == chunk - 1 else slot + 1
        after_block, after_wet = masked_at(after_slot)
        behind = pltpu.roll(block, 1, 1)
        after_ahead = pltpu.roll(after_block, cells - 1, 1)
        coming = jnp.where(slot == last, right_edge, after_ahead)
        sides = jnp.where(lane == 0, before, behind) + jnp.where(lane == cells - 1, coming, ahead)
        out[item] = (0.5 * sides + block) * (half_scale * wet)
        before, block, wet, ahead = behind, after_block, after_wet, after_ahead


def place(info, received, counts, capacity, fields, cells):
    steps = 4
    chunk = capacity // steps
    whole = pl.BlockSpec(memory_space=pltpu.VMEM)
    return pl.pallas_call(
        functools.partial(place_body, capacity=capacity),
        out_shape=jax.ShapeDtypeStruct((capacity, fields, cells), jnp.float32),
        grid=(steps,),
        in_specs=[pl.BlockSpec(memory_space=pltpu.SMEM), whole, whole],
        out_specs=pl.BlockSpec((chunk, fields, cells), lambda i: (i, 0, 0)),
        compiler_params=pltpu.CompilerParams(vmem_limit_bytes=SCRATCH_BYTES),
        name="place",
    )(info, in_vmem(received), in_vmem(counts))


def on_device(accum, step_count, stretch_slot, span_length, wet_mask):
    devices = lax.axis_size(AXES)
    me = lax.axis_index(AXES)
    blocks_dev, fields, cells = accum.shape
    capacity = wet_mask.shape[0]
    pair_most = capacity // devices
    all_blocks = stretch_slot.shape[0]
    windows = all_blocks // devices
    rows = pair_most * fields + TILE

    by_window = stretch_slot.reshape(windows, devices)
    here = by_window // blocks_dev == me
    ids = jnp.arange(all_blocks, dtype=jnp.int32).reshape(windows, devices)
    local = jnp.sum(jnp.where(here, by_window % blocks_dev, 0), axis=1)
    my_global = jnp.sum(jnp.where(here, ids, 0), axis=1)
    owner_ids = jnp.arange(devices, dtype=jnp.int32)
    edge_ids = jnp.arange(devices + 1, dtype=jnp.int32)
    starts = jnp.sum(jnp.where(owner_ids[None, :] < edge_ids[:, None], span_length[None, :], 0), axis=1)
    first_window = jnp.sum((my_global[None, :] < starts[:, None]).astype(jnp.int32), axis=1)
    table = jnp.concatenate([local, first_window])
    sendbuf = pack(table, accum, windows, devices, pair_most)
    received = lax.all_to_all(sendbuf, AXES, split_axis=0, concat_axis=0, tiled=True)
    received = received.reshape(devices * rows, cells)

    length = span_length[me]
    start = jnp.sum(jnp.where(owner_ids < me, span_length, 0))
    slots = jnp.arange(capacity, dtype=jnp.int32)
    valid = slots < length
    wet = jnp.where(valid & (wet_mask == 1), 1, 0)
    left_wet = passed_along(wet[length - 1], AXES, 1)
    right_wet = passed_along(wet[0], AXES, -1)
    padded = jnp.pad(stretch_slot, (1, capacity + 1))
    around = lax.dynamic_slice_in_dim(padded, start, capacity + 2) // blocks_dev
    sender = around[1:-1]
    opening = start // devices
    opening_senders = lax.dynamic_slice_in_dim(stretch_slot, opening * devices, devices) // blocks_dev
    skipped = (opening_senders[None, :] == sender[:, None]) & (owner_ids < start % devices)[None, :]
    rank = (start + slots) // devices - opening - jnp.sum(skipped.astype(jnp.int32), axis=1)
    row_of = jnp.where(valid, sender * rows + rank * fields, 0)
    edge_row = pair_most * fields
    left_row = around[0] * rows + edge_row
    right_row = jnp.sum(jnp.where(slots == length - 1, around[2:], 0)) * rows + edge_row
    facts = jnp.stack([left_wet, right_wet, length - 1, left_row, right_row])
    info = jnp.concatenate([row_of, wet, facts])
    return place(info, received, step_count.reshape(fields, 1), capacity, fields, cells)


def solution(mesh):
    return jax.shard_map(
        on_device,
        mesh=mesh,
        in_specs=(P(AXES, None, None), P(), P(), P(), P(AXES)),
        out_specs=P(AXES, None, None),
        check_vma=False,
    )
```
